32 devices in a mesh: gx: 4 (over y, x), gy: 8 (over z, core).
Axes of the slice: x: 2, y: 2, z: 4, core: 2. Of those that a mesh axis runs over, the one named last changes fastest.
Arguments:
- facets: float32 [2048, 12, 128], P(('gx', 'gy')), may hold values from -6 to 6
- owner: int32 [2048, 1], P(('gx', 'gy')), may hold values from 0 to 31; in each aligned block of 64 rows (0 to 63, 64 to 127, ...) at most 4 rows name the same one
- ghosts: int32 [32, 16], P(('gx', 'gy')), may hold values from 0 to 2047, as said below
- ghost_count: int32 [32], P(('gx', 'gy')), may hold values from 1 to 16, 256 in all
- nodes: float32 [3, 16384], P(None, ('gx', 'gy')), may hold values from -6 to 6
- cand: int32 [4, 16384], P(None, ('gx', 'gy')), may hold values from 0 to 15
Outputs:
- own_gap: float32 [16384], P(('gx', 'gy'))
- ghost_gap: float32 [16384], P(('gx', 'gy'))
The draws below stay inside these ranges and needn't reach their ends.
Inputs may be any that keep to these rules, and one draw needn't show every extreme that they name: Among the 64 blocks of one element-order device at most 4 have the same owner, and some owner reaches 4; every partition owns at least one block. `ghosts`: each row holds 16 distinct block ids. The blocks of element-order device h are h * 64 to h * 64 + 63; in every row exactly one device holds 2 of the entries and every other device holds at most one.
All inputs are finite; a program needn't handle non-finite values. No bound on the sum of `ghost_count` on one device may be relied on, other than what follows from the above.
Results may differ from the reference program's by a relative error of at most 0.0003.
Values sent between devices are 32-bit elements; how exact they have to be, the bound alone decides.
A program may use at most 64 MiB of HBM per device.

```python
import math
import jax
import jax.numpy as jnp
import numpy as np
from jax import lax

FB = 128
BPD = 64
ND = 512
CAP = 4
GH = 16
NC = 4
PARTS_SIZE = 32
NB = 2048
NODES = 16384
N_GX = 4
N_GY = 8


def draw_ghosts(key, part):

    def one_row(row_key):
        subkeys = jax.random.split(row_key, 4)
        holders = jax.random.permutation(subkeys[0], PARTS_SIZE)[:GH - 1].astype(jnp.int32)
        entry_holder = jnp.concatenate([holders[:1], holders])
        offsets = jax.random.randint(subkeys[1], (GH,), 0, BPD).astype(jnp.int32)
        stride = jax.random.randint(subkeys[2], (), 1, BPD).astype(jnp.int32)
        partner = (offsets[0] + stride) % BPD
        offsets = offsets.at[1].set(partner)
        block_ids = entry_holder * BPD + offsets
        shuffle = jax.random.permutation(subkeys[3], GH)
        return block_ids[shuffle]
    return jax.vmap(one_row)(jax.random.split(jax.random.fold_in(key, 11), PARTS_SIZE)).astype(jnp.int32)


def plant(drawn, own_key, least, top_value):
    place = [jax.random.randint(jax.random.fold_in(own_key, axis), (), 0, length) for axis, length in enumerate(drawn.shape)]
    widest = drawn.shape.index(max(drawn.shape))
    neighbour = place[:widest] + [(place[widest] + 1) % drawn.shape[widest]] + place[widest + 1:]
    return drawn.at[tuple(place)].set(least).at[tuple(neighbour)].set(top_value)


def block_scale(key, extent, cuts, low, largest):
    factor_of, own = 1.0, jax.random.fold_in(key, 6)
    for position, shards_of in cuts:
        heights = jnp.exp(jax.random.uniform(jax.random.fold_in(own, position), (shards_of,), jnp.float32, low / len(cuts), largest / len(cuts)))
        factor_of = factor_of * jnp.repeat(heights, extent[position] // shards_of).reshape([-1 if axis == position else 1 for axis in range(len(extent))])
    return factor_of


def profile(amount, total, bound, lean):
    loads = [(1 << 20) // math.isqrt(rank ** lean) + 1 for rank in range(2, amount + 1)]
    spare, given = total - bound - (amount - 1), [1] * (amount - 1)
    while spare > 0:
        candidates = [i for i in range(amount - 1) if given[i] < bound]
        whole, budget = sum([loads[i] for i in candidates]), spare
        for i in candidates:
            addition = min(bound - given[i], max(1, budget * loads[i] // whole), spare)
            given[i] = given[i] + addition
            spare = spare - addition
    return np.array([bound] + given)


def ragged_sizes(own_key, number_of, total, most, skew):
    if number_of == 2:
        one = jax.random.randint(own_key, (), max(1, total - most), min(most, total - 1) + 1)
        return jnp.stack([one, total - one])
    sizes = jnp.asarray(profile(number_of, total, most, skew), jnp.int32)
    pairs = (number_of - 1) // 2
    giver, sink = sizes[1:1 + 2 * pairs:2], sizes[2:2 + 2 * pairs:2]
    margin = jnp.minimum(giver - 1, most - sink)
    passed = jax.random.randint(jax.random.fold_in(own_key, 1), (pairs,), 0, 1 << 20) % (margin + 1)
    sizes = sizes.at[1:1 + 2 * pairs:2].set(giver - passed).at[2:2 + 2 * pairs:2].set(sink + passed)
    return sizes[jax.random.permutation(jax.random.fold_in(own_key, 2), number_of)]


def assign_block(key, own, number, rows, count, top, reach, lean):
    ranking = jax.random.permutation(key, count)
    heavy_load, ordinary = portions_of(count, rows * top, reach, lean, True), portions_of(count, rows * top, reach, lean, False)
    places = jnp.arange(count)

    def named(lengths, rotation):
        used = int((lengths > 0).sum())
        fixed = max(1, used // 4)
        shifted = fixed + (places - fixed + rotation * (used - fixed)) % max(1, count - fixed)
        return jnp.zeros((count,), jnp.int32).at[ranking[jnp.where(places < fixed, places, shifted)]].set(jnp.asarray(lengths, jnp.int32))

    lengths = jnp.where(number % 4 == 0, named(heavy_load, number // 4), named(ordinary, number - number // 4 - 1))
    mixed = jax.random.permutation(jax.random.fold_in(own, 3), count)
    source_of, taker = mixed[0:count // 2 * 2:2], mixed[1:count // 2 * 2:2]
    slack = jnp.minimum(lengths[source_of] - 1, reach - lengths[taker]) // 2
    slack = jnp.where((source_of == ranking[0]) | (taker == ranking[0]) | (lengths[taker] == 0), 0, jnp.maximum(slack, 0))
    shifted = jax.random.randint(jax.random.fold_in(own, 4), (count // 2,), 0, 1 << 20) % (slack + 1)
    lengths = lengths.at[source_of].add(-shifted).at[taker].add(shifted)
    items = jnp.searchsorted(jnp.cumsum(lengths), jnp.arange(rows * top), side="right").astype(jnp.int32)
    grid = items.reshape(top, rows).T
    grid = grid[jax.random.permutation(jax.random.fold_in(own, 1), rows)]
    rotation = jax.random.randint(jax.random.fold_in(own, 2), (rows, 1), 0, top)
    return jnp.take_along_axis(grid, (jnp.arange(top)[None, :] + rotation) % top, axis=1)


def portions_of(amount, total, most, lean, full):
    portions = [(1 << 20) // math.isqrt(rank ** lean) + 1 for rank in range(1, amount + 1)]
    largest = most if full else min(most, max(-(-total // amount), total * portions[0] // sum(portions)))
    least = 1 if total - largest >= amount - 1 else 0
    counts, surplus = [largest] + [least] * (amount - 1), total - largest - least * (amount - 1)
    while surplus > 0:
        free = [i for i in range(1, amount) if counts[i] < largest] or [i for i in range(1, amount) if counts[i] < most]
        pool, remaining = sum([portions[i] for i in free]), surplus
        for i in free:
            addition = min(most - counts[i], max(1, remaining * portions[i] // pool), surplus)
            counts[i] = counts[i] + addition
            surplus = surplus - addition
    return np.array(counts)


def normal_values(rng, shape, deviation, most, cuts=(), kind=jnp.bfloat16):
    values = deviation * jax.random.normal(rng, shape, jnp.float32)
    if cuts:
        values = values * block_scale(rng, shape, cuts, -0.22, 0.18)
    return jnp.clip(values, -most, most).astype(kind)


def setup_inputs(seed: int = 0) -> dict:
    key_of = jax.random.split(jax.random.key(seed), 7)
    facets = normal_values(key_of[0], (NB, 12, FB), 1.0, 6.0, ((0, 32),), jnp.float32)
    owner_keys = jax.random.split(jax.random.fold_in(key_of[1], 1), NB // BPD)
    owner_turns = jax.random.permutation(jax.random.fold_in(key_of[1], 3), NB // BPD)
    owner = jax.vmap(lambda own, number: assign_block(jax.random.fold_in(key_of[1], 2), own, number, BPD, PARTS_SIZE, 1, CAP, 2))(owner_keys, owner_turns).reshape((NB, 1))
    ghosts = draw_ghosts(jax.random.fold_in(key_of[6], 71), 0)
    ghost_count = ragged_sizes(key_of[3], PARTS_SIZE, PARTS_SIZE * GH // 2, GH, 2).astype(jnp.int32)
    nodes = normal_values(key_of[4], (3, NODES), 1.0, 6.0, ((1, 32),), jnp.float32)
    cand = plant(jax.random.randint(key_of[5], (NC, NODES), 0, GH), jax.random.fold_in(key_of[5], 1), 0, GH - 1).astype(jnp.int32)
    return dict(facets=facets, owner=owner, ghosts=ghosts, ghost_count=ghost_count, nodes=nodes, cand=cand)


far_gap = 10.0
penalty = 1.0e30


def facet_features(blocks, absent):
    vertex_a = blocks[:, 0:3]
    vertex_b = blocks[:, 3:6]
    vertex_c = blocks[:, 6:9]
    normal = blocks[:, 9:12]
    centre = (vertex_a + vertex_b + vertex_c) / 3.0
    spread = jnp.sum(vertex_a * vertex_a + vertex_b * vertex_b + vertex_c * vertex_c, axis=1) / 3.0
    offset = spread - jnp.sum(normal * vertex_a, axis=1) + penalty * absent[:, None]
    linear = normal - 2.0 * centre
    unit_row = jnp.ones_like(offset)
    stacked = jnp.concatenate([linear, unit_row[:, None], offset[:, None]], axis=1)
    return jnp.moveaxis(stacked, 1, 0).reshape(5, -1)


def node_features(points):
    square = jnp.sum(points * points, axis=0, keepdims=True)
    return jnp.concatenate([points, square, jnp.ones_like(square)], axis=0)


def pair_gaps(node_feat, facet_feat):
    return lax.dot_general(node_feat, facet_feat, (((0,), (0,)), ((), ())), precision=lax.Precision.HIGHEST, preferred_element_type=jnp.float32)


def reference(facets, owner, ghosts, ghost_count, nodes, cand):
    part_count = N_GX * N_GY
    slot_count = part_count * CAP
    target = owner[:, 0]
    per_part = jnp.moveaxis(nodes.reshape(3, part_count, ND), 1, 0)
    cand_part = jnp.moveaxis(cand.reshape(NC, part_count, ND), 1, 0)
    entries = jnp.arange(GH, dtype=jnp.int32)

    def one_part(operands):
        index, points, chosen, wanted, limit = operands
        node_feat = node_features(points)
        owned = target == index
        ordering = jnp.argsort(jnp.where(owned, 0, 1).astype(jnp.int32), stable=True)[:slot_count]
        absent = jnp.where(owned[ordering], 0.0, 1.0).astype(jnp.float32)
        own_min = jnp.min(pair_gaps(node_feat, facet_features(facets[ordering], absent)), axis=1)
        fetched = facets[wanted]
        gap_block = pair_gaps(node_feat, facet_features(fetched, jnp.zeros((GH,), jnp.float32))).reshape(ND, GH, FB)
        active = jnp.any((chosen[:, :, None] == entries[None, None, :]) & (entries[None, None, :] < limit), axis=0)
        ghost_min = jnp.minimum(far_gap, jnp.min(jnp.where(active[:, :, None], gap_block, penalty), axis=(1, 2)))
        return own_min, ghost_min

    own_min, ghost_min = lax.map(one_part, (jnp.arange(part_count, dtype=jnp.int32), per_part, cand_part, ghosts, ghost_count))
    return own_min.reshape(part_count * ND), ghost_min.reshape(part_count * ND)
```

```python
import functools

import jax
import jax.numpy as jnp
from jax import lax
from jax.experimental import pallas as pl
from jax.experimental.pallas import tpu as pltpu
from jax.sharding import PartitionSpec as P

CAP = 4
GC = 2
COMP = 4
LANES = 128

far_gap = 10.0
penalty = 1e30

MESH = pl.DeviceIdType.MESH


def split_terms(value):
    high = value.astype(jnp.bfloat16)
    rest = value - high.astype(jnp.float32)
    middle = rest.astype(jnp.bfloat16)
    low = (rest - middle.astype(jnp.float32)).astype(jnp.bfloat16)
    return high, middle, low


def facet_planes(planes):
    a, c, e, normal = (planes[0:3], planes[3:6], planes[6:9], planes[9:12])
    linear = [normal[i] - 2.0 * ((a[i] + c[i] + e[i]) / 3.0) for i in range(3)]
    spread = sum(a[i] * a[i] + c[i] * c[i] + e[i] * e[i] for i in range(3)) / 3.0
    offset = spread - sum(normal[i] * a[i] for i in range(3))
    return linear + [offset]


def lane_rows(row):
    return jnp.broadcast_to(row, (LANES, LANES)).T


def kernel(
    n_gx,
    n_gy,
    facets_ref,
    owner_ref,
    ghosts_ref,
    count_ref,
    nodes_ref,
    cand_ref,
    own_ref,
    ghost_ref,
    planes,
    own_send,
    own_recv,
    list_recv,
    reply_send,
    reply_recv,
    points,
    pens,
    entry_rows,
    own_acc,
    ghost_acc,
    load_sem,
    list_send_sem,
    list_recv_sem,
    own_send_sem,
    own_recv_sem,
    reply_send_sem,
    reply_recv_sem,
):
    n = n_gx * n_gy
    blocks = planes.shape[1]
    nodes = nodes_ref.shape[1]
    entries = ghosts_ref.shape[1]
    copies = LANES // blocks
    columns = COMP * blocks
    me = lax.axis_index("gx") * n_gy + lax.axis_index("gy")

    def coords(p):
        return (p // n_gy, p % n_gy)

    barrier = pltpu.get_barrier_semaphore()

    @pl.loop(1, n)
    def _(d):
        pl.semaphore_signal(
            barrier, inc=1, device_id=coords(lax.rem(me + d, n)), device_id_type=MESH
        )

    load = pltpu.make_async_copy(facets_ref, planes, load_sem)
    load.start()

    owner_row = jnp.concatenate([owner_ref[...]] * copies, axis=1)
    owner_col = lane_rows(owner_row)[0:blocks]
    lane = lax.broadcasted_iota(jnp.int32, (1, LANES), 1)
    place = lax.broadcasted_iota(jnp.int32, (blocks, LANES), 0)
    before = (owner_col == owner_row) & (place < lane % blocks)
    rank = jnp.sum(jnp.where(before, 1, 0), axis=0, keepdims=True)
    key = (owner_row * CAP + rank) * COMP + lane // blocks

    load.wait()
    features = facet_planes([planes[i] for i in range(12)])
    table = jnp.concatenate(features, axis=0)
    high, middle, low = split_terms(table)
    ones = jnp.ones((columns, LANES), jnp.bfloat16)
    stacked = jnp.concatenate([high, middle, low, ones], axis=1)

    tile = 128
    for start in range(0, n * CAP * COMP, tile):
        row = start + lax.broadcasted_iota(jnp.int32, (tile, LANES), 0)
        hot = jnp.concatenate(
            [jnp.where(row == key + i * copies, 1.0, 0.0) for i in range(COMP // copies)], axis=1
        ).astype(jnp.bfloat16)
        got = jnp.dot(hot, stacked, preferred_element_type=jnp.float32)
        value = got[:, 0:LANES] + got[:, LANES : 2 * LANES] + got[:, 2 * LANES : 3 * LANES]
        missing = (got[:, 3 * LANES :] == 0.0) & (row % COMP == COMP - 1)
        value = jnp.where(missing, penalty, value)
        per = tile // (CAP * COMP)
        own_send[start // (CAP * COMP) : start // (CAP * COMP) + per] = value.reshape(
            per, CAP * COMP, LANES
        )

    pl.semaphore_wait(barrier, n - 1)

    def list_copy(d):
        return pltpu.make_async_remote_copy(
            src_ref=ghosts_ref,
            dst_ref=list_recv.at[me],
            send_sem=list_send_sem,
            recv_sem=list_recv_sem,
            device_id=coords(lax.rem(me + d, n)),
            device_id_type=MESH,
        )

    def own_copy(d):
        target = lax.rem(me + d, n)
        return pltpu.make_async_remote_copy(
            src_ref=own_send.at[target],
            dst_ref=own_recv.at[me],
            send_sem=own_send_sem,
            recv_sem=own_recv_sem.at[me],
            device_id=coords(target),
            device_id_type=MESH,
        )

    def reply_copy(d):
        target = lax.rem(me + d, n)
        return pltpu.make_async_remote_copy(
            src_ref=reply_send.at[target],
            dst_ref=reply_recv.at[me],
            send_sem=reply_send_sem,
            recv_sem=reply_recv_sem,
            device_id=coords(target),
            device_id_type=MESH,
        )

    @pl.loop(1, n)
    def _(d):
        list_copy(d).start()

    @pl.loop(1, n)
    def _(d):
        own_copy(d).start()

    for start in range(0, nodes, LANES):
        rows = slice(start, start + LANES)
        for i in range(3):
            points[i, rows] = lane_rows(nodes_ref[i : i + 1, rows])
        chosen = [lane_rows(cand_ref[k : k + 1, rows]) for k in range(cand_ref.shape[0])]
        for e in range(entries):
            hit = functools.reduce(jnp.logical_or, [c == e for c in chosen])
            alive = jnp.where(e < count_ref[0], 0.0, penalty)
            pens[e, rows] = jnp.where(hit, alive, penalty)
    own_acc[...] = jnp.full(own_acc.shape, penalty, jnp.float32)

    wide = jnp.broadcast_to(ghosts_ref[...], (entries * COMP, entries))
    mine = lax.broadcasted_iota(jnp.int32, wide.shape, 1)
    rows_e = lax.broadcasted_iota(jnp.int32, wide.shape, 0)
    chosen_id = jnp.sum(jnp.where(mine == rows_e // COMP, wide, 0), axis=1, keepdims=True)
    holder = chosen_id // blocks
    larger = (wide // blocks == holder) & (wide > chosen_id)
    second = jnp.max(jnp.where(larger, 1, 0), axis=1, keepdims=True)
    component = lax.broadcasted_iota(jnp.int32, second.shape, 0) % COMP
    entry_rows[...] = jnp.broadcast_to(
        (holder * GC + second) * COMP + component, entry_rows.shape
    )

    list_recv[me] = ghosts_ref[...]
    pltpu.make_async_copy(
        list_recv.at[pl.ds(0, n - 1)], list_recv.at[pl.ds(0, n - 1)], list_recv_sem
    ).wait()
    group = 16
    for start in range(0, n, group):
        wanted = jnp.broadcast_to(list_recv[start : start + group], (group, 8, entries))
        local = wanted - me * blocks
        here = (local >= 0) & (local < blocks)
        far = 1 << 20
        first = jnp.max(jnp.where(here, local, -far), axis=2, keepdims=True)
        last = jnp.min(jnp.where(here, local, far), axis=2, keepdims=True)
        sub = lax.broadcasted_iota(jnp.int32, first.shape, 1)
        pick = jnp.where(sub < COMP, first, last) + (sub % COMP) * blocks
        pick = jnp.broadcast_to(pick, (group, 8, columns)).reshape(group * 8, columns)
        hot = jnp.where(
            pick == lax.broadcasted_iota(jnp.int32, (group * 8, columns), 1), 1.0, 0.0
        ).astype(jnp.bfloat16)
        got = jnp.dot(hot, stacked[:, 0 : 3 * LANES], preferred_element_type=jnp.float32)
        value = got[:, 0:LANES] + got[:, LANES : 2 * LANES] + got[:, 2 * LANES : 3 * LANES]
        reply_send[start : start + group] = value.reshape(group, 8, LANES)

    @pl.loop(1, n)
    def _(d):
        reply_copy(d).start()

    reply_recv[me] = reply_send[me]
    own_recv[me] = own_send[me]

    step = 64

    def own_chunk(source):
        chunk = own_recv[source]
        parts = [[chunk[COMP * c + k : COMP * c + k + 1] for k in range(COMP)] for c in range(CAP)]
        for start in range(0, nodes, step):
            rows = slice(start, start + step)
            x, y, z = points[0, rows], points[1, rows], points[2, rows]
            best = own_acc[rows]
            for lx, ly, lz, offset in parts:
                best = jnp.minimum(best, (x * lx + offset) + (y * ly + z * lz))
            own_acc[rows] = best

    own_chunk(me)

    @pl.loop(1, n)
    def _(d):
        source = lax.rem(me + n - d, n)
        pltpu.make_async_copy(
            own_recv.at[source], own_recv.at[source], own_recv_sem.at[source]
        ).wait()
        own_chunk(source)

    square = jnp.sum(nodes_ref[...] * nodes_ref[...], axis=0, keepdims=True)
    for start in range(0, nodes, LANES):
        rows = slice(start, start + LANES)
        least = jnp.min(own_acc[rows].T, axis=0, keepdims=True)
        own_ref[:, rows] = least + square[:, rows]

    pltpu.make_async_copy(
        reply_recv.at[pl.ds(0, n - 1)], reply_recv.at[pl.ds(0, n - 1)], reply_recv_sem
    ).wait()
    reply = reply_recv[...].reshape(n * GC * COMP, LANES)
    spot = lax.broadcasted_iota(jnp.int32, (entries * COMP, n * GC * COMP), 1)
    target_row = jnp.broadcast_to(entry_rows[:, 0:1], spot.shape)
    hot = jnp.where(target_row == spot, 1.0, 0.0).astype(jnp.bfloat16)
    got = jnp.dot(
        hot, jnp.concatenate(split_terms(reply), axis=1), preferred_element_type=jnp.float32
    )
    fetched = got[:, 0:LANES] + got[:, LANES : 2 * LANES] + got[:, 2 * LANES : 3 * LANES]
    ghost_acc[...] = fetched
    for start in range(0, nodes, LANES):
        bests = []
        for inner in range(start, start + LANES, 32):
            rows = slice(inner, inner + 32)
            x, y, z = points[0, rows], points[1, rows], points[2, rows]
            best = jnp.full((32, LANES), penalty, jnp.float32)
            for e in range(entries):
                lx, ly, lz, offset = [
                    ghost_acc[COMP * e + k : COMP * e + k + 1] for k in range(COMP)
                ]
                gap = (x * lx + offset) + (y * ly + z * lz)
                best = jnp.minimum(best, gap + pens[e, rows])
            bests.append(best)
        rows = slice(start, start + LANES)
        least = jnp.min(jnp.concatenate(bests, axis=0).T, axis=0, keepdims=True)
        ghost_ref[:, rows] = jnp.minimum(far_gap, least + square[:, rows])

    def all_of(ref, sem):
        pltpu.make_async_copy(ref.at[pl.ds(0, n - 1)], ref.at[pl.ds(0, n - 1)], sem).wait()

    all_of(list_recv, list_send_sem)
    all_of(own_recv, own_send_sem)
    all_of(reply_recv, reply_send_sem)


def solution(mesh):
    n_gx, n_gy = mesh.shape["gx"], mesh.shape["gy"]
    n = n_gx * n_gy

    def local(facets, owner, ghosts, ghost_count, nodes, cand):
        blocks, width = facets.shape[0], facets.shape[2]
        node_count = nodes.shape[1]
        entries = ghosts.shape[1]
        vmem = pl.BlockSpec(memory_space=pltpu.VMEM)
        own, ghost = pl.pallas_call(
            functools.partial(kernel, n_gx, n_gy),
            out_shape=[jax.ShapeDtypeStruct((1, node_count), jnp.float32)] * 2,
            in_specs=[
                pl.BlockSpec(memory_space=pl.ANY),
                vmem,
                vmem,
                pl.BlockSpec(memory_space=pltpu.SMEM),
                vmem,
                vmem,
            ],
            out_specs=[vmem, vmem],
            scratch_shapes=[
                pltpu.VMEM((12, blocks, width), jnp.float32),
                pltpu.VMEM((n, CAP * COMP, width), jnp.float32),
                pltpu.VMEM((n, CAP * COMP, width), jnp.float32),
                pltpu.VMEM((n, 1, entries), jnp.int32),
                pltpu.VMEM((n, GC * COMP, width), jnp.float32),
                pltpu.VMEM((n, GC * COMP, width), jnp.float32),
                pltpu.VMEM((3, node_count, width), jnp.float32),
                pltpu.VMEM((entries, node_count, width), jnp.float32),
                pltpu.VMEM((entries * COMP, width), jnp.int32),
                pltpu.VMEM((node_count, width), jnp.float32),
                pltpu.VMEM((entries * COMP, width), jnp.float32),
                pltpu.SemaphoreType.DMA,
                pltpu.SemaphoreType.DMA,
                pltpu.SemaphoreType.DMA,
                pltpu.SemaphoreType.DMA,
                pltpu.SemaphoreType.DMA((n,)),
                pltpu.SemaphoreType.DMA,
                pltpu.SemaphoreType.DMA,
            ],
            compiler_params=pltpu.CompilerParams(collective_id=0, has_side_effects=True),
        )(
            jnp.transpose(facets, (1, 0, 2)),
            owner.reshape(1, blocks),
            ghosts,
            ghost_count,
            nodes,
            cand,
        )
        return own.reshape(node_count), ghost.reshape(node_count)

    return jax.shard_map(
        local,
        mesh=mesh,
        in_specs=(
            P(("gx", "gy"), None, None),
            P(("gx", "gy"), None),
            P(("gx", "gy"), None),
            P(("gx", "gy")),
            P(None, ("gx", "gy")),
            P(None, ("gx", "gy")),
        ),
        out_specs=(P(("gx", "gy")), P(("gx", "gy"))),
        check_vma=False,
    )
```

```python
import functools

import jax
import jax.numpy as jnp
from jax import lax
from jax.experimental import pallas as pl
from jax.experimental.pallas import tpu as pltpu
from jax.sharding import PartitionSpec as P

CAP = 4
GC = 2
COMP = 4
LANES = 128

far_gap = 10.0
penalty = 1e30

MESH = pl.DeviceIdType.MESH


def split_terms(value):
    high = value.astype(jnp.bfloat16)
    rest = value - high.astype(jnp.float32)
    middle = rest.astype(jnp.bfloat16)
    low = (rest - middle.astype(jnp.float32)).astype(jnp.bfloat16)
    return high, middle, low


def facet_planes(planes):
    a, c, e, normal = (planes[0:3], planes[3:6], planes[6:9], planes[9:12])
    linear = [normal[i] - 2.0 * ((a[i] + c[i] + e[i]) / 3.0) for i in range(3)]
    spread = sum(a[i] * a[i] + c[i] * c[i] + e[i] * e[i] for i in range(3)) / 3.0
    offset = spread - sum(normal[i] * a[i] for i in range(3))
    return linear + [offset]


def lane_rows(row):
    return jnp.broadcast_to(row, (LANES, LANES)).T


def kernel(
    n_gx,
    n_gy,
    facets_hbm,
    owner_hbm,
    ghosts_hbm,
    count_hbm,
    nodes_hbm,
    cand_hbm,
    own_ref,
    ghost_ref,
    planes,
    owner_ref,
    ghosts_ref,
    count_ref,
    nodes_ref,
    cand_ref,
    own_send,
    own_recv,
    list_recv,
    reply_send,
    reply_recv,
    points,
    pens,
    entry_rows,
    own_acc,
    ghost_acc,
    load_sem,
    list_send_sem,
    list_recv_sem,
    own_send_sem,
    own_recv_sem,
    reply_send_sem,
    reply_recv_sem,
):
    n = n_gx * n_gy
    blocks = planes.shape[1]
    nodes = nodes_ref.shape[1]
    entries = ghosts_ref.shape[1]
    copies = LANES // blocks
    columns = COMP * blocks
    my_x, my_y = lax.axis_index("gx"), lax.axis_index("gy")
    me = my_x * n_gy + my_y
    pair = 2 if n_gy % 2 == 0 else 1
    pairs = n_gy // pair
    my_pair, my_side = lax.div(my_y, pair), lax.rem(my_y, pair)

    def wrap(value, size):
        value = jnp.where(value >= size, value - size, value)
        return jnp.where(value < 0, value + size, value)

    def peer(j, dx, flip, sign):
        side = my_side if flip == 0 else pair - 1 - my_side
        return wrap(my_x + sign * dx, n_gx), wrap(my_pair + sign * j, pairs) * pair + side

    def near(body):
        for flip in range(1, pair):
            body(0, 0, flip)

        @pl.loop(1, n_gx)
        def _(dx):
            for flip in range(pair):
                body(0, dx, flip)

    def far(body):
        @pl.loop(1, pairs)
        def _(j):
            @pl.loop(0, n_gx)
            def _(dx):
                for flip in range(pair):
                    body(j, dx, flip)

    barrier = pltpu.get_barrier_semaphore()

    def greet(j, dx, flip):
        pl.semaphore_signal(
            barrier, inc=1, device_id=peer(j, dx, flip, 1), device_id_type=MESH
        )

    far(greet)
    near(greet)

    load = pltpu.make_async_copy(facets_hbm, planes, load_sem.at[0])
    small = [
        pltpu.make_async_copy(source, target, load_sem.at[1 + i])
        for i, (source, target) in enumerate(
            [
                (owner_hbm, owner_ref),
                (ghosts_hbm, ghosts_ref),
                (count_hbm, count_ref),
                (nodes_hbm, nodes_ref),
                (cand_hbm, cand_ref),
            ]
        )
    ]
    for copy in small:
        copy.start()
    load.start()
    for copy in small:
        copy.wait()

    count = count_ref[...]
    for start in range(0, nodes, LANES):
        rows = slice(start, start + LANES)
        for i in range(3):
            points[i, rows] = lane_rows(nodes_ref[i : i + 1, rows])
        chosen = [lane_rows(cand_ref[k : k + 1, rows]) for k in range(cand_ref.shape[0])]
        for e in range(entries):
            hit = functools.reduce(jnp.logical_or, [c == e for c in chosen])
            alive = jnp.where(e < count, 0.0, penalty)
            pens[e, rows] = jnp.where(hit, alive, penalty)
    own_acc[...] = jnp.full(own_acc.shape, penalty, jnp.float32)

    wide = jnp.broadcast_to(ghosts_ref[...], (entries * COMP, entries))
    mine = lax.broadcasted_iota(jnp.int32, wide.shape, 1)
    rows_e = lax.broadcasted_iota(jnp.int32, wide.shape, 0)
    chosen_id = jnp.sum(jnp.where(mine == rows_e // COMP, wide, 0), axis=1, keepdims=True)
    holder = chosen_id // blocks
    larger = (wide // blocks == holder) & (wide > chosen_id)
    second = jnp.max(jnp.where(larger, 1, 0), axis=1, keepdims=True)
    component = lax.broadcasted_iota(jnp.int32, second.shape, 0) % COMP
    entry_rows[...] = jnp.broadcast_to(
        (holder * GC + second) * COMP + component, entry_rows.shape
    )

    owner_row = jnp.concatenate([owner_ref[...]] * copies, axis=1)
    owner_col = lane_rows(owner_row)[0:blocks]
    lane = lax.broadcasted_iota(jnp.int32, (1, LANES), 1)
    place = lax.broadcasted_iota(jnp.int32, (blocks, LANES), 0)
    before = (owner_col == owner_row) & (place < lane % blocks)
    rank = jnp.sum(jnp.where(before, 1, 0), axis=0, keepdims=True)
    key = (owner_row * CAP + rank) * COMP + lane // blocks

    load.wait()
    features = facet_planes([planes[i] for i in range(12)])
    table = jnp.concatenate(features, axis=0)
    high, middle, low = split_terms(table)
    ones = jnp.ones((columns, LANES), jnp.bfloat16)
    stacked = jnp.concatenate([high, middle, low, ones], axis=1)

    tile = 128
    for start in range(0, n * CAP * COMP, tile):
        row = start + lax.broadcasted_iota(jnp.int32, (tile, LANES), 0)
        hot = jnp.concatenate(
            [jnp.where(row == key + i * copies, 1.0, 0.0) for i in range(COMP // copies)], axis=1
        ).astype(jnp.bfloat16)
        got = jnp.dot(hot, stacked, preferred_element_type=jnp.float32)
        value = got[:, 0:LANES] + got[:, LANES : 2 * LANES] + got[:, 2 * LANES : 3 * LANES]
        missing = (got[:, 3 * LANES :] == 0.0) & (row % COMP == COMP - 1)
        value = jnp.where(missing, penalty, value)
        per = tile // (CAP * COMP)
        own_send[start // (CAP * COMP) : start // (CAP * COMP) + per] = value.reshape(
            per, CAP * COMP, LANES
        )

    pl.semaphore_wait(barrier, n - 1)

    def send(source, target, send_sem, recv_sem):
        def start(j, dx, flip):
            to_x, to_y = peer(j, dx, flip, 1)
            pltpu.make_async_remote_copy(
                src_ref=source(to_x * n_gy + to_y),
                dst_ref=target.at[me],
                send_sem=send_sem,
                recv_sem=recv_sem,
                device_id=(to_x, to_y),
                device_id_type=MESH,
            ).start()

        return start

    list_start = send(lambda p: ghosts_ref, list_recv, list_send_sem, list_recv_sem)
    own_start = send(lambda p: own_send.at[p], own_recv, own_send_sem, own_recv_sem.at[me])
    reply_start = send(lambda p: reply_send.at[p], reply_recv, reply_send_sem, reply_recv_sem)

    far(list_start)
    near(list_start)
    near(own_start)
    far(own_start)

    step = 64

    def own_chunk(source):
        chunk = own_recv[source]
        parts = [[chunk[COMP * c + k : COMP * c + k + 1] for k in range(COMP)] for c in range(CAP)]
        for start in range(0, nodes, step):
            rows = slice(start, start + step)
            x, y, z = points[0, rows], points[1, rows], points[2, rows]
            best = own_acc[rows]
            for lx, ly, lz, offset in parts:
                best = jnp.minimum(best, (x * lx + offset) + (y * ly + z * lz))
            own_acc[rows] = best

    def own_take(j, dx, flip):
        from_x, from_y = peer(j, dx, flip, -1)
        source = from_x * n_gy + from_y
        pltpu.make_async_copy(
            own_recv.at[source], own_recv.at[source], own_recv_sem.at[source]
        ).wait()
        own_chunk(source)

    own_recv[me] = own_send[me]
    own_chunk(me)
    near(own_take)

    list_recv[me] = ghosts_ref[...]
    pltpu.make_async_copy(
        list_recv.at[pl.ds(0, n - 1)], list_recv.at[pl.ds(0, n - 1)], list_recv_sem
    ).wait()
    group = 16
    for start in range(0, n, group):
        wanted = jnp.broadcast_to(list_recv[start : start + group], (group, 8, entries))
        local = wanted - me * blocks
        here = (local >= 0) & (local < blocks)
        outside = 1 << 20
        first = jnp.max(jnp.where(here, local, -outside), axis=2, keepdims=True)
        last = jnp.min(jnp.where(here, local, outside), axis=2, keepdims=True)
        sub = lax.broadcasted_iota(jnp.int32, first.shape, 1)
        pick = jnp.where(sub < COMP, first, last) + (sub % COMP) * blocks
        pick = jnp.broadcast_to(pick, (group, 8, columns)).reshape(group * 8, columns)
        hot = jnp.where(
            pick == lax.broadcasted_iota(jnp.int32, (group * 8, columns), 1), 1.0, 0.0
        ).astype(jnp.bfloat16)
        got = jnp.dot(hot, stacked[:, 0 : 3 * LANES], preferred_element_type=jnp.float32)
        value = got[:, 0:LANES] + got[:, LANES : 2 * LANES] + got[:, 2 * LANES : 3 * LANES]
        reply_send[start : start + group] = value.reshape(group, 8, LANES)

    far(reply_start)
    near(reply_start)
    reply_recv[me] = reply_send[me]
    far(own_take)
    square = jnp.sum(nodes_ref[...] * nodes_ref[...], axis=0, keepdims=True)
    for start in range(0, nodes, LANES):
        rows = slice(start, start + LANES)
        least = jnp.min(own_acc[rows].T, axis=0, keepdims=True)
        own_ref[rows] = (least + square[:, rows]).reshape(LANES)

    pltpu.make_async_copy(
        reply_recv.at[pl.ds(0, n - 1)], reply_recv.at[pl.ds(0, n - 1)], reply_recv_sem
    ).wait()
    reply = reply_recv[...].reshape(n * GC * COMP, LANES)
    spot = lax.broadcasted_iota(jnp.int32, (entries * COMP, n * GC * COMP), 1)
    target_row = jnp.broadcast_to(entry_rows[:, 0:1], spot.shape)
    hot = jnp.where(target_row == spot, 1.0, 0.0).astype(jnp.bfloat16)
    got = jnp.dot(
        hot, jnp.concatenate(split_terms(reply), axis=1), preferred_element_type=jnp.float32
    )
    fetched = got[:, 0:LANES] + got[:, LANES : 2 * LANES] + got[:, 2 * LANES : 3 * LANES]
    ghost_acc[...] = fetched
    for start in range(0, nodes, LANES):
        bests = []
        for inner in range(start, start + LANES, 32):
            rows = slice(inner, inner + 32)
            x, y, z = points[0, rows], points[1, rows], points[2, rows]
            best = jnp.full((32, LANES), penalty, jnp.float32)
            for e in range(entries):
                lx, ly, lz, offset = [
                    ghost_acc[COMP * e + k : COMP * e + k + 1] for k in range(COMP)
                ]
                gap = (x * lx + offset) + (y * ly + z * lz)
                best = jnp.minimum(best, gap + pens[e, rows])
            bests.append(best)
        rows = slice(start, start + LANES)
        least = jnp.min(jnp.concatenate(bests, axis=0).T, axis=0, keepdims=True)
        ghost_ref[rows] = jnp.minimum(far_gap, least + square[:, rows]).reshape(LANES)

    def all_of(ref, sem):
        pltpu.make_async_copy(ref.at[pl.ds(0, n - 1)], ref.at[pl.ds(0, n - 1)], sem).wait()

    all_of(list_recv, list_send_sem)
    all_of(own_recv, own_send_sem)
    all_of(reply_recv, reply_send_sem)


def solution(mesh):
    n_gx, n_gy = mesh.shape["gx"], mesh.shape["gy"]
    n = n_gx * n_gy

    def local(facets, owner, ghosts, ghost_count, nodes, cand):
        blocks, width = facets.shape[0], facets.shape[2]
        node_count = nodes.shape[1]
        entries = ghosts.shape[1]
        vmem = pl.BlockSpec(memory_space=pltpu.VMEM)
        own, ghost = pl.pallas_call(
            functools.partial(kernel, n_gx, n_gy),
            out_shape=[jax.ShapeDtypeStruct((node_count,), jnp.float32)] * 2,
            in_specs=[pl.BlockSpec(memory_space=pl.ANY)] * 6,
            out_specs=[vmem, vmem],
            scratch_shapes=[
                pltpu.VMEM((12, blocks, width), jnp.float32),
                pltpu.VMEM((1, blocks), jnp.int32),
                pltpu.VMEM((1, entries), jnp.int32),
                pltpu.VMEM((1, 1), jnp.int32),
                pltpu.VMEM((3, node_count), jnp.float32),
                pltpu.VMEM((cand.shape[0], node_count), jnp.int32),
                pltpu.VMEM((n, CAP * COMP, width), jnp.float32),
                pltpu.VMEM((n, CAP * COMP, width), jnp.float32),
                pltpu.VMEM((n, 1, entries), jnp.int32),
                pltpu.VMEM((n, GC * COMP, width), jnp.float32),
                pltpu.VMEM((n, GC * COMP, width), jnp.float32),
                pltpu.VMEM((3, node_count, width), jnp.float32),
                pltpu.VMEM((entries, node_count, width), jnp.float32),
                pltpu.VMEM((entries * COMP, width), jnp.int32),
                pltpu.VMEM((node_count, width), jnp.float32),
                pltpu.VMEM((entries * COMP, width), jnp.float32),
                pltpu.SemaphoreType.DMA((6,)),
                pltpu.SemaphoreType.DMA,
                pltpu.SemaphoreType.DMA,
                pltpu.SemaphoreType.DMA,
                pltpu.SemaphoreType.DMA((n,)),
                pltpu.SemaphoreType.DMA,
                pltpu.SemaphoreType.DMA,
            ],
            compiler_params=pltpu.CompilerParams(collective_id=0, has_side_effects=True),
        )(
            jnp.transpose(facets, (1, 0, 2)),
            owner.reshape(1, blocks),
            ghosts,
            ghost_count.reshape(1, 1),
            nodes,
            cand,
        )
        return own, ghost

    return jax.shard_map(
        local,
        mesh=mesh,
        in_specs=(
            P(("gx", "gy"), None, None),
            P(("gx", "gy"), None),
            P(("gx", "gy"), None),
            P(("gx", "gy")),
            P(None, ("gx", "gy")),
            P(None, ("gx", "gy")),
        ),
        out_specs=(P(("gx", "gy")), P(("gx", "gy"))),
        check_vma=False,
    )
```

```python
import functools

import jax
import jax.numpy as jnp
from jax import lax
from jax.experimental import pallas as pl
from jax.experimental.pallas import tpu as pltpu
from jax.sharding import PartitionSpec as P

CAP = 4
GC = 2
COMP = 4
LANES = 128

far_gap = 10.0
penalty = 1e30

MESH = pl.DeviceIdType.MESH


def split_terms(value):
    high = value.astype(jnp.bfloat16)
    rest = value - high.astype(jnp.float32)
    middle = rest.astype(jnp.bfloat16)
    low = (rest - middle.astype(jnp.float32)).astype(jnp.bfloat16)
    return high, middle, low


def facet_planes(planes):
    a, c, e, normal = (planes[0:3], planes[3:6], planes[6:9], planes[9:12])
    linear = [normal[i] - 2.0 * ((a[i] + c[i] + e[i]) / 3.0) for i in range(3)]
    spread = sum(a[i] * a[i] + c[i] * c[i] + e[i] * e[i] for i in range(3)) / 3.0
    offset = spread - sum(normal[i] * a[i] for i in range(3))
    return linear + [offset]


def lane_rows(row):
    return jnp.broadcast_to(row, (LANES, LANES)).T


def kernel(
    n_gx,
    n_gy,
    facets_hbm,
    owner_hbm,
    ghosts_hbm,
    count_hbm,
    nodes_hbm,
    cand_hbm,
    own_ref,
    ghost_ref,
    planes,
    owner_ref,
    ghosts_ref,
    count_ref,
    nodes_ref,
    cand_ref,
    own_send,
    own_recv,
    list_recv,
    reply_send,
    reply_recv,
    points,
    pens,
    entry_rows,
    ids_ref,
    own_acc,
    ghost_acc,
    load_sem,
    list_send_sem,
    list_recv_sem,
    own_send_sem,
    own_recv_sem,
    reply_send_sem,
    reply_recv_sem,
):
    n = n_gx * n_gy
    blocks = planes.shape[1]
    nodes = nodes_ref.shape[1]
    entries = ghosts_ref.shape[1]
    copies = LANES // blocks
    columns = COMP * blocks
    my_x, my_y = lax.axis_index("gx"), lax.axis_index("gy")
    me = my_x * n_gy + my_y
    pair = 2 if n_gy % 2 == 0 else 1
    pairs = n_gy // pair
    my_pair, my_side = lax.div(my_y, pair), lax.rem(my_y, pair)

    def wrap(value, size):
        value = jnp.where(value >= size, value - size, value)
        return jnp.where(value < 0, value + size, value)

    def peer(j, dx, flip, sign):
        side = my_side if flip == 0 else pair - 1 - my_side
        return wrap(my_x + sign * dx, n_gx), wrap(my_pair + sign * j, pairs) * pair + side

    def near(body):
        for flip in range(1, pair):
            body(0, 0, flip)

        @pl.loop(1, n_gx)
        def _(dx):
            for flip in range(pair):
                body(0, dx, flip)

    def far(body):
        @pl.loop(1, pairs)
        def _(j):
            @pl.loop(0, n_gx)
            def _(dx):
                for flip in range(pair):
                    body(j, dx, flip)

    barrier = pltpu.get_barrier_semaphore()

    def greet(j, dx, flip):
        pl.semaphore_signal(
            barrier, inc=1, device_id=peer(j, dx, flip, 1), device_id_type=MESH
        )

    far(greet)
    near(greet)

    load = pltpu.make_async_copy(facets_hbm, planes, load_sem.at[0])
    small = [
        pltpu.make_async_copy(source, target, load_sem.at[1 + i])
        for i, (source, target) in enumerate(
            [
                (owner_hbm, owner_ref),
                (ghosts_hbm, ghosts_ref),
                (ghosts_hbm, ids_ref),
                (count_hbm, count_ref),
                (nodes_hbm, nodes_ref),
                (cand_hbm, cand_ref),
            ]
        )
    ]
    for copy in small:
        copy.start()
    load.start()
    for copy in small:
        copy.wait()

    owner_row = jnp.concatenate([owner_ref[...]] * copies, axis=1)
    owner_col = lane_rows(owner_row)[0:blocks]
    lane = lax.broadcasted_iota(jnp.int32, (1, LANES), 1)
    place = lax.broadcasted_iota(jnp.int32, (blocks, LANES), 0)
    before = (owner_col == owner_row) & (place < lane % blocks)
    rank = jnp.sum(jnp.where(before, 1, 0), axis=0, keepdims=True)
    key = (owner_row * CAP + rank) * COMP + lane // blocks

    load.wait()
    features = facet_planes([planes[i] for i in range(12)])
    table = jnp.concatenate(features, axis=0)
    high, middle, low = split_terms(table)
    ones = jnp.ones((columns, LANES), jnp.bfloat16)
    stacked = jnp.concatenate([high, middle, low, ones], axis=1)

    tile = 128
    for start in range(0, n * CAP * COMP, tile):
        row = start + lax.broadcasted_iota(jnp.int32, (tile, LANES), 0)
        hot = jnp.concatenate(
            [jnp.where(row == key + i * copies, 1.0, 0.0) for i in range(COMP // copies)], axis=1
        ).astype(jnp.bfloat16)
        got = jnp.dot(hot, stacked, preferred_element_type=jnp.float32)
        value = got[:, 0:LANES] + got[:, LANES : 2 * LANES] + got[:, 2 * LANES : 3 * LANES]
        missing = (got[:, 3 * LANES :] == 0.0) & (row % COMP == COMP - 1)
        value = jnp.where(missing, penalty, value)
        per = tile // (CAP * COMP)
        own_send[start // (CAP * COMP) : start // (CAP * COMP) + per] = value.reshape(
            per, CAP * COMP, LANES
        )

    pl.semaphore_wait(barrier, n - 1)

    def send(source, target, send_sem, recv_sem):
        def start(j, dx, flip):
            to_x, to_y = peer(j, dx, flip, 1)
            pltpu.make_async_remote_copy(
                src_ref=source(to_x * n_gy + to_y),
                dst_ref=target.at[me],
                send_sem=send_sem,
                recv_sem=recv_sem,
                device_id=(to_x, to_y),
                device_id_type=MESH,
            ).start()

        return start

    list_start = send(lambda p: ghosts_ref, list_recv, list_send_sem, list_recv_sem)
    own_start = send(lambda p: own_send.at[p], own_recv, own_send_sem, own_recv_sem.at[me])
    reply_start = send(lambda p: reply_send.at[p], reply_recv, reply_send_sem, reply_recv_sem)

    far(list_start)
    near(list_start)
    near(own_start)
    far(own_start)

    count = count_ref[0]
    for start in range(0, nodes, LANES):
        rows = slice(start, start + LANES)
        for i in range(3):
            points[i, rows] = lane_rows(nodes_ref[i : i + 1, rows])
        chosen = [lane_rows(cand_ref[k : k + 1, rows]) for k in range(cand_ref.shape[0])]
        for e in range(entries):
            hit = functools.reduce(jnp.logical_or, [c == e for c in chosen])
            alive = jnp.where(e < count, 0.0, penalty)
            pens[e, rows] = jnp.where(hit, alive, penalty)
    own_acc[...] = jnp.full(own_acc.shape, penalty, jnp.float32)

    wide = jnp.broadcast_to(ghosts_ref[...], (entries * COMP, entries))
    mine = lax.broadcasted_iota(jnp.int32, wide.shape, 1)
    rows_e = lax.broadcasted_iota(jnp.int32, wide.shape, 0)
    chosen_id = jnp.sum(jnp.where(mine == rows_e // COMP, wide, 0), axis=1, keepdims=True)
    larger = (wide // blocks == chosen_id // blocks) & (wide > chosen_id)
    second = jnp.max(jnp.where(larger, 1, 0), axis=1, keepdims=True)
    entry_rows[...] = jnp.broadcast_to(second, entry_rows.shape)

    step = 64

    def own_chunk(source):
        chunk = own_recv[source]
        parts = [[chunk[COMP * c + k : COMP * c + k + 1] for k in range(COMP)] for c in range(CAP)]
        for start in range(0, nodes, step):
            rows = slice(start, start + step)
            x, y, z = points[0, rows], points[1, rows], points[2, rows]
            best = own_acc[rows]
            for lx, ly, lz, offset in parts:
                best = jnp.minimum(best, (x * lx + offset) + (y * ly + z * lz))
            own_acc[rows] = best

    def own_take(j, dx, flip):
        from_x, from_y = peer(j, dx, flip, -1)
        source = from_x * n_gy + from_y
        pltpu.make_async_copy(
            own_recv.at[source], own_recv.at[source], own_recv_sem.at[source]
        ).wait()
        own_chunk(source)

    own_recv[me] = own_send[me]
    own_chunk(me)
    near(own_take)

    list_recv[me] = ghosts_ref[...]
    pltpu.make_async_copy(
        list_recv.at[pl.ds(0, n - 1)], list_recv.at[pl.ds(0, n - 1)], list_recv_sem
    ).wait()
    group = 16
    for start in range(0, n, group):
        wanted = jnp.broadcast_to(list_recv[start : start + group], (group, 8, entries))
        local = wanted - me * blocks
        here = (local >= 0) & (local < blocks)
        outside = 1 << 20
        first = jnp.max(jnp.where(here, local, -outside), axis=2, keepdims=True)
        last = jnp.min(jnp.where(here, local, outside), axis=2, keepdims=True)
        sub = lax.broadcasted_iota(jnp.int32, first.shape, 1)
        pick = jnp.where(sub < COMP, first, last) + (sub % COMP) * blocks
        pick = jnp.broadcast_to(pick, (group, 8, columns)).reshape(group * 8, columns)
        hot = jnp.where(
            pick == lax.broadcasted_iota(jnp.int32, (group * 8, columns), 1), 1.0, 0.0
        ).astype(jnp.bfloat16)
        got = jnp.dot(hot, stacked[:, 0 : 3 * LANES], preferred_element_type=jnp.float32)
        value = got[:, 0:LANES] + got[:, LANES : 2 * LANES] + got[:, 2 * LANES : 3 * LANES]
        reply_send[start : start + group] = value.reshape(group, 8, LANES)

    far(reply_start)
    near(reply_start)
    reply_recv[me] = reply_send[me]
    far(own_take)
    square = jnp.sum(nodes_ref[...] * nodes_ref[...], axis=0, keepdims=True)
    for start in range(0, nodes, LANES):
        rows = slice(start, start + LANES)
        least = jnp.min(own_acc[rows].T, axis=0, keepdims=True)
        own_ref[rows] = (least + square[:, rows]).reshape(LANES)

    pltpu.make_async_copy(
        reply_recv.at[pl.ds(0, n - 1)], reply_recv.at[pl.ds(0, n - 1)], reply_recv_sem
    ).wait()
    for e in range(entries):
        block = reply_recv[lax.div(ids_ref[0, e], blocks)]
        rows = slice(COMP * e, COMP * e + COMP)
        ghost_acc[rows] = jnp.where(entry_rows[rows] == 1, block[COMP:], block[0:COMP])
    for start in range(0, nodes, LANES):
        bests = []
        for inner in range(start, start + LANES, 32):
            rows = slice(inner, inner + 32)
            x, y, z = points[0, rows], points[1, rows], points[2, rows]
            best = jnp.full((32, LANES), penalty, jnp.float32)
            for e in range(entries):
                lx, ly, lz, offset = [
                    ghost_acc[COMP * e + k : COMP * e + k + 1] for k in range(COMP)
                ]
                gap = (x * lx + offset) + (y * ly + z * lz)
                best = jnp.minimum(best, gap + pens[e, rows])
            bests.append(best)
        rows = slice(start, start + LANES)
        least = jnp.min(jnp.concatenate(bests, axis=0).T, axis=0, keepdims=True)
        ghost_ref[rows] = jnp.minimum(far_gap, least + square[:, rows]).reshape(LANES)

    def all_of(ref, sem):
        pltpu.make_async_copy(ref.at[pl.ds(0, n - 1)], ref.at[pl.ds(0, n - 1)], sem).wait()

    all_of(list_recv, list_send_sem)
    all_of(own_recv, own_send_sem)
    all_of(reply_recv, reply_send_sem)


def solution(mesh):
    n_gx, n_gy = mesh.shape["gx"], mesh.shape["gy"]
    n = n_gx * n_gy

    def local(facets, owner, ghosts, ghost_count, nodes, cand):
        blocks, width = facets.shape[0], facets.shape[2]
        node_count = nodes.shape[1]
        entries = ghosts.shape[1]
        vmem = pl.BlockSpec(memory_space=pltpu.VMEM)
        own, ghost = pl.pallas_call(
            functools.partial(kernel, n_gx, n_gy),
            out_shape=[pltpu.VMEM((node_count,), jnp.float32)] * 2,
            in_specs=[pl.BlockSpec(memory_space=pl.ANY)] * 6,
            out_specs=[vmem, vmem],
            scratch_shapes=[
                pltpu.VMEM((12, blocks, width), jnp.float32),
                pltpu.VMEM((1, blocks), jnp.int32),
                pltpu.VMEM((1, entries), jnp.int32),
                pltpu.SMEM((1,), jnp.int32),
                pltpu.VMEM((3, node_count), jnp.float32),
                pltpu.VMEM((cand.shape[0], node_count), jnp.int32),
                pltpu.VMEM((n, CAP * COMP, width), jnp.float32),
                pltpu.VMEM((n, CAP * COMP, width), jnp.float32),
                pltpu.VMEM((n, 1, entries), jnp.int32),
                pltpu.VMEM((n, GC * COMP, width), jnp.float32),
                pltpu.VMEM((n, GC * COMP, width), jnp.float32),
                pltpu.VMEM((3, node_count, width), jnp.float32),
                pltpu.VMEM((entries, node_count, width), jnp.float32),
                pltpu.VMEM((entries * COMP, width), jnp.int32),
                pltpu.SMEM((1, entries), jnp.int32),
                pltpu.VMEM((node_count, width), jnp.float32),
                pltpu.VMEM((entries * COMP, width), jnp.float32),
                pltpu.SemaphoreType.DMA((7,)),
                pltpu.SemaphoreType.DMA,
                pltpu.SemaphoreType.DMA,
                pltpu.SemaphoreType.DMA,
                pltpu.SemaphoreType.DMA((n,)),
                pltpu.SemaphoreType.DMA,
                pltpu.SemaphoreType.DMA,
            ],
            compiler_params=pltpu.CompilerParams(collective_id=0, has_side_effects=True),
        )(
            jnp.transpose(facets, (1, 0, 2)),
            owner.reshape(1, blocks),
            ghosts,
            ghost_count,
            nodes,
            cand,
        )
        return own, ghost

    return jax.shard_map(
        local,
        mesh=mesh,
        in_specs=(
            P(("gx", "gy"), None, None),
            P(("gx", "gy"), None),
            P(("gx", "gy"), None),
            P(("gx", "gy")),
            P(None, ("gx", "gy")),
            P(None, ("gx", "gy")),
        ),
        out_specs=(P(("gx", "gy")), P(("gx", "gy"))),
        check_vma=False,
    )
```

```python
import functools

import jax
import jax.numpy as jnp
from jax import lax
from jax.experimental import pallas as pl
from jax.experimental.pallas import tpu as pltpu
from jax.sharding import PartitionSpec as P

CAP = 4
GC = 2
COMP = 4
LANES = 128

far_gap = 10.0
penalty = 1e30

MESH = pl.DeviceIdType.MESH


def split_terms(value):
    high = value.astype(jnp.bfloat16)
    rest = value - high.astype(jnp.float32)
    middle = rest.astype(jnp.bfloat16)
    low = (rest - middle.astype(jnp.float32)).astype(jnp.bfloat16)
    return high, middle, low


def facet_planes(planes):
    a, c, e, normal = (planes[0:3], planes[3:6], planes[6:9], planes[9:12])
    linear = [normal[i] - 2.0 * ((a[i] + c[i] + e[i]) / 3.0) for i in range(3)]
    spread = sum(a[i] * a[i] + c[i] * c[i] + e[i] * e[i] for i in range(3)) / 3.0
    offset = spread - sum(normal[i] * a[i] for i in range(3))
    return linear + [offset]


def lane_rows(row):
    return jnp.broadcast_to(row, (LANES, LANES)).T


def kernel(
    n_gx,
    n_gy,
    facets_hbm,
    owner_hbm,
    ghosts_hbm,
    count_hbm,
    nodes_hbm,
    cand_hbm,
    own_ref,
    ghost_ref,
    planes,
    owner_ref,
    ghosts_ref,
    count_ref,
    nodes_ref,
    cand_ref,
    own_send,
    own_recv,
    list_recv,
    reply_send,
    reply_recv,
    points,
    pens,
    entry_rows,
    ids_ref,
    own_acc,
    ghost_acc,
    load_sem,
    list_send_sem,
    list_recv_sem,
    own_send_sem,
    own_recv_sem,
    reply_send_sem,
    reply_recv_sem,
):
    n = n_gx * n_gy
    blocks = planes.shape[1]
    nodes = nodes_ref.shape[1]
    entries = ghosts_ref.shape[1]
    copies = LANES // blocks
    columns = COMP * blocks
    my_x, my_y = lax.axis_index("gx"), lax.axis_index("gy")
    me = my_x * n_gy + my_y
    pair = 2 if n_gy % 2 == 0 else 1
    pairs = n_gy // pair
    my_pair, my_side = lax.div(my_y, pair), lax.rem(my_y, pair)

    def wrap(value, size):
        value = jnp.where(value >= size, value - size, value)
        return jnp.where(value < 0, value + size, value)

    def peer(j, dx, flip, sign):
        side = my_side if flip == 0 else pair - 1 - my_side
        return wrap(my_x + sign * dx, n_gx), wrap(my_pair + sign * j, pairs) * pair + side

    def near(body):
        for flip in range(1, pair):
            body(0, 0, flip)

        @pl.loop(1, n_gx)
        def _(dx):
            for flip in range(pair):
                body(0, dx, flip)

    def far(body):
        @pl.loop(1, pairs)
        def _(j):
            @pl.loop(0, n_gx)
            def _(dx):
                for flip in range(pair):
                    body(j, dx, flip)

    def every(body):
        for j in list(range(1, pairs)) + [0]:
            for dx in range(n_gx):
                for flip in range(pair):
                    if j or dx or flip:
                        body(j, dx, flip)

    barrier = pltpu.get_barrier_semaphore()

    def greet(j, dx, flip):
        pl.semaphore_signal(
            barrier, inc=1, device_id=peer(j, dx, flip, 1), device_id_type=MESH
        )

    every(greet)

    load = pltpu.make_async_copy(facets_hbm, planes, load_sem.at[0])
    small = [
        pltpu.make_async_copy(source, target, load_sem.at[1 + i])
        for i, (source, target) in enumerate(
            [
                (owner_hbm, owner_ref),
                (ghosts_hbm, ghosts_ref),
                (ghosts_hbm, ids_ref),
                (count_hbm, count_ref),
                (nodes_hbm, nodes_ref),
                (cand_hbm, cand_ref),
            ]
        )
    ]
    for copy in small:
        copy.start()
    load.start()
    for copy in small:
        copy.wait()

    owner_row = jnp.concatenate([owner_ref[...]] * copies, axis=1)
    owner_col = lane_rows(owner_row)[0:blocks]
    lane = lax.broadcasted_iota(jnp.int32, (1, LANES), 1)
    place = lax.broadcasted_iota(jnp.int32, (blocks, LANES), 0)
    before = (owner_col == owner_row) & (place < lane % blocks)
    rank = jnp.sum(jnp.where(before, 1, 0), axis=0, keepdims=True)
    key = (owner_row * CAP + rank) * COMP + lane // blocks

    load.wait()
    features = facet_planes([planes[i] for i in range(12)])
    table = jnp.concatenate(features, axis=0)
    high, middle, low = split_terms(table)
    ones = jnp.ones((columns, LANES), jnp.bfloat16)
    stacked = jnp.concatenate([high, middle, low, ones], axis=1)

    tile = 128
    for start in range(0, n * CAP * COMP, tile):
        row = start + lax.broadcasted_iota(jnp.int32, (tile, LANES), 0)
        hot = jnp.concatenate(
            [jnp.where(row == key + i * copies, 1.0, 0.0) for i in range(COMP // copies)], axis=1
        ).astype(jnp.bfloat16)
        got = jnp.dot(hot, stacked, preferred_element_type=jnp.float32)
        value = got[:, 0:LANES] + got[:, LANES : 2 * LANES] + got[:, 2 * LANES : 3 * LANES]
        missing = (got[:, 3 * LANES :] == 0.0) & (row % COMP == COMP - 1)
        value = jnp.where(missing, penalty, value)
        per = tile // (CAP * COMP)
        own_send[start // (CAP * COMP) : start // (CAP * COMP) + per] = value.reshape(
            per, CAP * COMP, LANES
        )

    pl.semaphore_wait(barrier, n - 1)

    def send(source, target, send_sem, recv_sem):
        def start(j, dx, flip):
            to_x, to_y = peer(j, dx, flip, 1)
            pltpu.make_async_remote_copy(
                src_ref=source(to_x * n_gy + to_y),
                dst_ref=target.at[me],
                send_sem=send_sem,
                recv_sem=recv_sem,
                device_id=(to_x, to_y),
                device_id_type=MESH,
            ).start()

        return start

    list_start = send(lambda p: ghosts_ref, list_recv, list_send_sem, list_recv_sem)
    own_start = send(lambda p: own_send.at[p], own_recv, own_send_sem, own_recv_sem.at[me])
    reply_start = send(lambda p: reply_send.at[p], reply_recv, reply_send_sem, reply_recv_sem)

    every(list_start)
    every(own_start)

    count = count_ref[0]
    for start in range(0, nodes, LANES):
        rows = slice(start, start + LANES)
        for i in range(3):
            points[i, rows] = lane_rows(nodes_ref[i : i + 1, rows])
        chosen = [lane_rows(cand_ref[k : k + 1, rows]) for k in range(cand_ref.shape[0])]
        for e in range(entries):
            hit = functools.reduce(jnp.logical_or, [c == e for c in chosen])
            alive = jnp.where(e < count, 0.0, penalty)
            pens[e, rows] = jnp.where(hit, alive, penalty)
    own_acc[...] = jnp.full(own_acc.shape, penalty, jnp.float32)

    wide = jnp.broadcast_to(ghosts_ref[...], (entries * COMP, entries))
    mine = lax.broadcasted_iota(jnp.int32, wide.shape, 1)
    rows_e = lax.broadcasted_iota(jnp.int32, wide.shape, 0)
    chosen_id = jnp.sum(jnp.where(mine == rows_e // COMP, wide, 0), axis=1, keepdims=True)
    larger = (wide // blocks == chosen_id // blocks) & (wide > chosen_id)
    second = jnp.max(jnp.where(larger, 1, 0), axis=1, keepdims=True)
    entry_rows[...] = jnp.broadcast_to(second, entry_rows.shape)

    step = 64

    def own_chunk(source):
        chunk = own_recv[source]
        parts = [[chunk[COMP * c + k : COMP * c + k + 1] for k in range(COMP)] for c in range(CAP)]
        for start in range(0, nodes, step):
            rows = slice(start, start + step)
            x, y, z = points[0, rows], points[1, rows], points[2, rows]
            best = own_acc[rows]
            for lx, ly, lz, offset in parts:
                best = jnp.minimum(best, (x * lx + offset) + (y * ly + z * lz))
            own_acc[rows] = best

    def own_take(j, dx, flip):
        from_x, from_y = peer(j, dx, flip, -1)
        source = from_x * n_gy + from_y
        pltpu.make_async_copy(
            own_recv.at[source], own_recv.at[source], own_recv_sem.at[source]
        ).wait()
        own_chunk(source)

    own_recv[me] = own_send[me]
    own_chunk(me)
    near(own_take)

    list_recv[me] = ghosts_ref[...]
    pltpu.make_async_copy(
        list_recv.at[pl.ds(0, n - 1)], list_recv.at[pl.ds(0, n - 1)], list_recv_sem
    ).wait()
    group = 16
    for start in range(0, n, group):
        wanted = jnp.broadcast_to(list_recv[start : start + group], (group, 8, entries))
        local = wanted - me * blocks
        here = (local >= 0) & (local < blocks)
        outside = 1 << 20
        first = jnp.max(jnp.where(here, local, -outside), axis=2, keepdims=True)
        last = jnp.min(jnp.where(here, local, outside), axis=2, keepdims=True)
        sub = lax.broadcasted_iota(jnp.int32, first.shape, 1)
        pick = jnp.where(sub < COMP, first, last) + (sub % COMP) * blocks
        pick = jnp.broadcast_to(pick, (group, 8, columns)).reshape(group * 8, columns)
        hot = jnp.where(
            pick == lax.broadcasted_iota(jnp.int32, (group * 8, columns), 1), 1.0, 0.0
        ).astype(jnp.bfloat16)
        got = jnp.dot(hot, stacked[:, 0 : 3 * LANES], preferred_element_type=jnp.float32)
        value = got[:, 0:LANES] + got[:, LANES : 2 * LANES] + got[:, 2 * LANES : 3 * LANES]
        reply_send[start : start + group] = value.reshape(group, 8, LANES)

    every(reply_start)
    reply_recv[me] = reply_send[me]
    far(own_take)
    square = jnp.sum(nodes_ref[...] * nodes_ref[...], axis=0, keepdims=True)
    for start in range(0, nodes, LANES):
        rows = slice(start, start + LANES)
        least = jnp.min(own_acc[rows].T, axis=0, keepdims=True)
        own_ref[rows] = (least + square[:, rows]).reshape(LANES)

    pltpu.make_async_copy(
        reply_recv.at[pl.ds(0, n - 1)], reply_recv.at[pl.ds(0, n - 1)], reply_recv_sem
    ).wait()
    for e in range(entries):
        block = reply_recv[lax.div(ids_ref[0, e], blocks)]
        rows = slice(COMP * e, COMP * e + COMP)
        ghost_acc[rows] = jnp.where(entry_rows[rows] == 1, block[COMP:], block[0:COMP])
    for start in range(0, nodes, LANES):
        bests = []
        for inner in range(start, start + LANES, 32):
            rows = slice(inner, inner + 32)
            x, y, z = points[0, rows], points[1, rows], points[2, rows]
            best = jnp.full((32, LANES), penalty, jnp.float32)
            for e in range(entries):
                lx, ly, lz, offset = [
                    ghost_acc[COMP * e + k : COMP * e + k + 1] for k in range(COMP)
                ]
                gap = (x * lx + offset) + (y * ly + z * lz)
                best = jnp.minimum(best, gap + pens[e, rows])
            bests.append(best)
        rows = slice(start, start + LANES)
        least = jnp.min(jnp.concatenate(bests, axis=0).T, axis=0, keepdims=True)
        ghost_ref[rows] = jnp.minimum(far_gap, least + square[:, rows]).reshape(LANES)

    def all_of(ref, sem):
        pltpu.make_async_copy(ref.at[pl.ds(0, n - 1)], ref.at[pl.ds(0, n - 1)], sem).wait()

    all_of(list_recv, list_send_sem)
    all_of(own_recv, own_send_sem)
    all_of(reply_recv, reply_send_sem)


def solution(mesh):
    n_gx, n_gy = mesh.shape["gx"], mesh.shape["gy"]
    n = n_gx * n_gy

    def local(facets, owner, ghosts, ghost_count, nodes, cand):
        blocks, width = facets.shape[0], facets.shape[2]
        node_count = nodes.shape[1]
        entries = ghosts.shape[1]
        vmem = pl.BlockSpec(memory_space=pltpu.VMEM)
        own, ghost = pl.pallas_call(
            functools.partial(kernel, n_gx, n_gy),
            out_shape=[pltpu.VMEM((node_count,), jnp.float32)] * 2,
            in_specs=[pl.BlockSpec(memory_space=pl.ANY)] * 6,
            out_specs=[vmem, vmem],
            scratch_shapes=[
                pltpu.VMEM((12, blocks, width), jnp.float32),
                pltpu.VMEM((1, blocks), jnp.int32),
                pltpu.VMEM((1, entries), jnp.int32),
                pltpu.SMEM((1,), jnp.int32),
                pltpu.VMEM((3, node_count), jnp.float32),
                pltpu.VMEM((cand.shape[0], node_count), jnp.int32),
                pltpu.VMEM((n, CAP * COMP, width), jnp.float32),
                pltpu.VMEM((n, CAP * COMP, width), jnp.float32),
                pltpu.VMEM((n, 1, entries), jnp.int32),
                pltpu.VMEM((n, GC * COMP, width), jnp.float32),
                pltpu.VMEM((n, GC * COMP, width), jnp.float32),
                pltpu.VMEM((3, node_count, width), jnp.float32),
                pltpu.VMEM((entries, node_count, width), jnp.float32),
                pltpu.VMEM((entries * COMP, width), jnp.int32),
                pltpu.SMEM((1, entries), jnp.int32),
                pltpu.VMEM((node_count, width), jnp.float32),
                pltpu.VMEM((entries * COMP, width), jnp.float32),
                pltpu.SemaphoreType.DMA((7,)),
                pltpu.SemaphoreType.DMA,
                pltpu.SemaphoreType.DMA,
                pltpu.SemaphoreType.DMA,
                pltpu.SemaphoreType.DMA((n,)),
                pltpu.SemaphoreType.DMA,
                pltpu.SemaphoreType.DMA,
            ],
            compiler_params=pltpu.CompilerParams(collective_id=0, has_side_effects=True),
        )(
            jnp.transpose(facets, (1, 0, 2)),
            owner.reshape(1, blocks),
            ghosts,
            ghost_count,
            nodes,
            cand,
        )
        return own, ghost

    return jax.shard_map(
        local,
        mesh=mesh,
        in_specs=(
            P(("gx", "gy"), None, None),
            P(("gx", "gy"), None),
            P(("gx", "gy"), None),
            P(("gx", "gy")),
            P(None, ("gx", "gy")),
            P(None, ("gx", "gy")),
        ),
        out_specs=(P(("gx", "gy")), P(("gx", "gy"))),
        check_vma=False,
    )
```
